32 devices in a mesh: blk: 8 (over z, x), grp: 4 (over y, core).
Axes of the slice: x: 2, y: 2, z: 4, core: 2. Of those that a mesh axis runs over, the one named last changes fastest.
Arguments:
- source_coords: float32 [3, 20480], P(None, ('blk', 'grp')), may hold values from 0 to 8, as said below
- source_values: float32 [3, 20480], P(None, ('blk', 'grp')), may hold values from -48 to 48
- target_coords: float32 [3, 16384], P(None, ('blk', 'grp')), may hold values from 0 to 8, as said below
- target_owner: int32 [16384], P(('blk', 'grp')), may hold values from 0 to 7, as said below
Outputs:
- weights: float32 [3, 20480], P(None, ('blk', 'grp'))
- poly: float32 [3, 4], replicated
- mapped: float32 [3, 16384], P(None, ('blk', 'grp'))
The draws below stay inside these ranges and needn't reach their ends.
Inputs may be any that keep to these rules, and one draw needn't show every extreme that they name: `source_coords`: source vertex j has its first coordinate between j // 2560 and j // 2560 + 1, and the other two between 0 and 1. `target_coords`: target vertex t has its first coordinate between target_owner[t] and target_owner[t] + 1, and the other two between 0 and 1. target_owner[t] differs from t // 2048 by at most one.
All inputs are finite; a program needn't handle non-finite values.
Results may differ from the reference program's by a relative error of at most 0.0003.
Values sent between devices are 32-bit elements; how exact they have to be, the bound alone decides.
A program may use at most 64 MiB of HBM per device.

```python
import math
import jax
import jax.numpy as jnp
from jax import lax

C = 3
ITERS = 3
REACH = 2
TGT_DEV = 512
SLAB = 2560
NSRC = 20480
NTGT = 16384
N_BLK = 8
N_GRP = 4


def spread_draw(key, count):
    spread = jax.random.uniform(key, (3, count), jnp.float32)
    return spread


def source_layout(key):
    count = SLAB * N_BLK
    slab = (jnp.arange(count, dtype=jnp.int32) // SLAB).astype(jnp.float32)
    spread = spread_draw(jax.random.fold_in(key, 101), count)
    return jnp.stack([slab + spread[0], spread[1], spread[2]])


def draw_source_coords(key, part):
    return source_layout(key)


def draw_source_values(key, part):
    coords = source_layout(key)
    count = coords.shape[1]
    ones = jnp.ones_like(coords[0])
    basis_rows = jnp.stack([ones, 2.0 * coords[0] / N_BLK - 1.0, 2.0 * coords[1] - 1.0, 2.0 * coords[2] - 1.0])
    rising = 1.0 + 2.0 * coords[0] / N_BLK
    trend = jax.random.uniform(jax.random.fold_in(key, 202), (C, 4), jnp.float32, -1.5, 1.5)
    rough = jnp.clip(jax.random.normal(jax.random.fold_in(key, 203), (C, count), jnp.float32), -4.0, 4.0)
    return jnp.dot(trend, basis_rows) + rising[None, :] * rough


def target_layout(key):
    count = TGT_DEV * N_GRP * N_BLK
    home = jnp.arange(count, dtype=jnp.int32) // (TGT_DEV * N_GRP)
    offset = jax.random.randint(jax.random.fold_in(key, 303), (count,), -1, 2)
    return jnp.clip(home + offset, 0, N_BLK - 1)


def draw_target_owner(key, part):
    return target_layout(key).astype(jnp.int32)


def draw_target_coords(key, part):
    owner = target_layout(key).astype(jnp.float32)
    count = owner.shape[0]
    spread = spread_draw(jax.random.fold_in(key, 404), count)
    return jnp.stack([owner + spread[0], spread[1], spread[2]])


def setup_inputs(seed: int = 0) -> dict:
    key_of = jax.random.split(jax.random.key(seed), 5)
    source_coords = draw_source_coords(jax.random.fold_in(key_of[4], 71), 0)
    source_values = draw_source_values(jax.random.fold_in(key_of[4], 71), 0)
    target_coords = draw_target_coords(jax.random.fold_in(key_of[4], 71), 0)
    target_owner = draw_target_owner(jax.random.fold_in(key_of[4], 71), 0)
    return {"source_coords": source_coords, "source_values": source_values, "target_coords": target_coords, "target_owner": target_owner}


precise = lax.Precision.HIGHEST
thin_factor = 0.6
tiny = 1e-06

def kernel_tile(rows, cols, stretch):
    along = rows[0][None, :] - cols[0][:, None]
    across = rows[1][None, :] - cols[1][:, None]
    upward = rows[2][None, :] - cols[2][:, None]
    return jnp.exp(-(thin_factor * along * along + stretch * (across * across + upward * upward)))

def basis(points, partitions, sources):
    ones = jnp.ones_like(points[0])
    stacked = jnp.stack([ones, 2.0 * points[0] / partitions - 1.0, 2.0 * points[1] - 1.0, 2.0 * points[2] - 1.0])
    return stacked / math.sqrt(sources)

def least_squares(hessenberg, beta):
    count = len(hessenberg)
    right_side = [beta] + [jnp.zeros_like(beta) for k in range(count)]
    upper = []
    cosines = []
    sines = []
    for k in range(count):
        column = list(hessenberg[k])
        for i in range(k):
            top = cosines[i] * column[i] + sines[i] * column[i + 1]
            lower = -sines[i] * column[i] + cosines[i] * column[i + 1]
            column[i] = top
            column[i + 1] = lower
        radius = jnp.sqrt(column[k] * column[k] + column[k + 1] * column[k + 1])
        cosine = column[k] / radius
        sine = column[k + 1] / radius
        column[k] = radius
        cosines.append(cosine)
        sines.append(sine)
        right_side[k + 1] = -sine * right_side[k]
        right_side[k] = cosine * right_side[k]
        upper.append(column[:k + 1])
    solved = [None] * count
    for k in reversed(range(count)):
        running = right_side[k]
        for j in range(k + 1, count):
            running = running - upper[j][k] * solved[j]
        solved[k] = running / upper[k][k]
    return solved

def reference(source_coords, source_values, target_coords, target_owner):
    stretch = 4.0 * SLAB
    reach = REACH
    poly_src = basis(source_coords, N_BLK, NSRC)
    margin = reach * SLAB
    coords_pad = jnp.pad(source_coords, ((0, 0), (margin, margin)))

    def kernel_apply(head):
        head_pad = jnp.pad(head, ((0, 0), (margin, margin)))

        def one_slab(slab):
            start = (slab * SLAB).astype(jnp.int32)
            rows = lax.dynamic_slice_in_dim(source_coords, start, SLAB, 1)
            running = jnp.zeros((C, SLAB), jnp.float32)
            for offset in range(2 * reach + 1):
                begin = (start + offset * SLAB).astype(jnp.int32)
                cols = lax.dynamic_slice_in_dim(coords_pad, begin, SLAB, 1)
                values = lax.dynamic_slice_in_dim(head_pad, begin, SLAB, 1)
                running = running + jnp.dot(values, kernel_tile(rows, cols, stretch), precision=precise, preferred_element_type=jnp.float32)
            return running
        blocks = lax.map(one_slab, jnp.arange(N_BLK, dtype=jnp.int32))
        return jnp.transpose(blocks, (1, 0, 2)).reshape(C, NSRC)

    def operate(head, tail):
        image_head = kernel_apply(head) + jnp.dot(tail, poly_src, precision=precise, preferred_element_type=jnp.float32)
        image_tail = jnp.dot(head, poly_src.T, precision=precise, preferred_element_type=jnp.float32)
        return (image_head, image_tail)
    beta = jnp.sqrt(lax.optimization_barrier(jnp.sum(source_values * source_values, axis=1)) + tiny)
    heads = [source_values / beta[:, None]]
    tails = [jnp.zeros((C, 4), jnp.float32)]
    hessenberg = []
    for k in range(ITERS):
        image_head, image_tail = operate(heads[k], tails[k])
        column = []
        for i in range(k + 1):
            column.append(lax.optimization_barrier(jnp.sum(heads[i] * image_head, axis=1)) + lax.optimization_barrier(jnp.sum(tails[i] * image_tail, axis=1)))
        rest_head = image_head
        rest_tail = image_tail
        for i in range(k + 1):
            rest_head = rest_head - column[i][:, None] * heads[i]
            rest_tail = rest_tail - column[i][:, None] * tails[i]
        length = jnp.sqrt(lax.optimization_barrier(jnp.sum(rest_head * rest_head, axis=1)) + lax.optimization_barrier(jnp.sum(rest_tail * rest_tail, axis=1)) + tiny)
        column.append(length)
        hessenberg.append(column)
        heads.append(rest_head / length[:, None])
        tails.append(rest_tail / length[:, None])
    solved = least_squares(hessenberg, beta)
    weights = solved[0][:, None] * heads[0]
    poly = solved[0][:, None] * tails[0]
    for k in range(1, ITERS):
        weights = weights + solved[k][:, None] * heads[k]
        poly = poly + solved[k][:, None] * tails[k]
    poly_tgt = basis(target_coords, N_BLK, NSRC)
    wide = (reach + 1) * SLAB
    coords_far = jnp.pad(source_coords, ((0, 0), (wide, wide)))
    weights_far = jnp.pad(weights, ((0, 0), (wide, wide)))
    group_rows = TGT_DEV * N_GRP

    def one_group(group):
        first = (group * group_rows).astype(jnp.int32)
        rows = lax.dynamic_slice_in_dim(target_coords, first, group_rows, 1)
        owners = lax.dynamic_slice_in_dim(target_owner, first, group_rows, 0)
        running = jnp.zeros((C, group_rows), jnp.float32)
        for offset in range(2 * reach + 3):
            slab = group + offset - reach - 1
            begin = ((group + offset) * SLAB).astype(jnp.int32)
            cols = lax.dynamic_slice_in_dim(coords_far, begin, SLAB, 1)
            values = lax.dynamic_slice_in_dim(weights_far, begin, SLAB, 1)
            tile = kernel_tile(rows, cols, stretch)
            tile = jnp.where((jnp.abs(owners - slab) <= reach)[None, :], tile, 0.0)
            running = running + jnp.dot(values, tile, precision=precise, preferred_element_type=jnp.float32)
        return running
    evaluated = lax.map(one_group, jnp.arange(N_BLK, dtype=jnp.int32))
    mapped = jnp.transpose(evaluated, (1, 0, 2)).reshape(C, NTGT)
    mapped = mapped + jnp.dot(poly, poly_tgt, precision=precise, preferred_element_type=jnp.float32)
    return (weights, poly, mapped)
```

```python
import functools
import math

import jax
import jax.numpy as jnp
from jax import lax
from jax.experimental import pallas as pl
from jax.experimental.pallas import tpu as pltpu
from jax.sharding import PartitionSpec as P

ITERS = 3
REACH = 2
C = 3
thin_factor = 0.6
tiny = 1e-06
LANES = 128
GROUP = 64
MESH = pl.DeviceIdType.MESH


def least_squares(hessenberg, beta):
    count = len(hessenberg)
    right_side = [beta] + [jnp.zeros_like(beta) for k in range(count)]
    upper, cosines, sines = [], [], []
    for k in range(count):
        column = list(hessenberg[k])
        for i in range(k):
            top = cosines[i] * column[i] + sines[i] * column[i + 1]
            lower = -sines[i] * column[i] + cosines[i] * column[i + 1]
            column[i] = top
            column[i + 1] = lower
        radius = jnp.sqrt(column[k] * column[k] + column[k + 1] * column[k + 1])
        cosine = column[k] / radius
        sine = column[k + 1] / radius
        column[k] = radius
        cosines.append(cosine)
        sines.append(sine)
        right_side[k + 1] = -sine * right_side[k]
        right_side[k] = cosine * right_side[k]
        upper.append(column[: k + 1])
    solved = [None] * count
    for k in reversed(range(count)):
        running = right_side[k]
        for j in range(k + 1, count):
            running = running - upper[j][k] * solved[j]
        solved[k] = running / upper[k][k]
    return solved


def kernel(
    n_blk, n_grp, sub, tsub, scale_x, scale_y, root_n,
    own_ref, tgt_ref, out_w, out_m, out_p,
    kbuf, rowb, accb, recv0, recv1, recv2, recv3, send0, send1, send2, send3,
    ccols, v0, v1, v2, wn, send_sem, recv_sem,
):
    blk = lax.axis_index("blk")
    grp = lax.axis_index("grp")
    peers = n_blk * n_grp
    wide = REACH + 1
    near = (2 * wide + 1) * n_grp
    recvs = (recv0, recv1, recv2, recv3)
    sends = (send0, send1, send2, send3)
    heads = (v0, v1, v2)
    own_near = wide * n_grp

    def target(p):
        e = p // n_grp
        h = p % n_grp
        return lax.rem(blk + e, n_blk), lax.rem(grp + h, n_grp), e

    barrier = pltpu.get_barrier_semaphore()

    def greet(p, carry):
        tb, tg, e = target(p)
        pl.semaphore_signal(barrier, inc=1, device_id=(tb, tg), device_id_type=MESH)
        return carry

    lax.fori_loop(1, peers, greet, 0)

    lane = lax.broadcasted_iota(jnp.int32, (1, LANES), 1)
    sub8 = lax.broadcasted_iota(jnp.int32, (8, LANES), 0)
    sub16 = lax.broadcasted_iota(jnp.int32, (16, LANES), 0)

    def rows16(f):
        return jnp.where(sub16 < sub, f[0:1], jnp.where(sub16 < 2 * sub, f[1:2], f[2:3]))

    x_own = own_ref[0:sub]
    y_own = own_ref[sub : 2 * sub]
    z_own = own_ref[2 * sub : 3 * sub]

    def basis_rows(x, y, z):
        return (
            jnp.full_like(x, 1.0 / root_n),
            (x * (2.0 / (n_blk * scale_x)) - 1.0) * (1.0 / root_n),
            y * (2.0 / (scale_y * root_n)),
            z * (2.0 / (scale_y * root_n)),
        )

    p_own = basis_rows(x_own, y_own, z_own)

    def total(a):
        return jnp.sum(jnp.sum(a, axis=0, keepdims=True), axis=1, keepdims=True)

    def dots_row(w, others):
        row = jnp.zeros((1, LANES), jnp.float32)
        for c in range(C):
            wc = w[c * sub : (c + 1) * sub]
            terms = [(i, total(wc * o[c * sub : (c + 1) * sub])) for i, o in enumerate(others)]
            terms.append((3, total(wc * wc)))
            terms += [(4 + j, total(wc * p_own[j])) for j in range(4)]
            for q, value in terms:
                row = jnp.where(lane == 16 * c + q, value, row)
        return row

    vals = own_ref[16:32]
    row0 = dots_row(vals, [])
    send0[0:16] = own_ref[0:16]
    send0[16:31] = own_ref[16:31]
    send0[31:32] = row0
    pl.semaphore_wait(barrier, peers - 1)

    def copy_to(r, p):
        tb, tg, e = target(p)
        return pltpu.make_async_remote_copy(
            src_ref=sends[r],
            dst_ref=recvs[r].at[p],
            send_sem=send_sem.at[r],
            recv_sem=recv_sem.at[r],
            device_id=(tb, tg),
            device_id_type=MESH,
        )

    def start_round(r):
        def body(p, carry):
            copy_to(r, p).start()
            return carry

        lax.fori_loop(1, peers, body, 0)
        recvs[r][0] = sends[r][...]

    def wait_round(r):
        landed = recvs[r].at[pl.ds(1, peers - 1)]
        pltpu.make_async_copy(landed, landed, recv_sem.at[r]).wait()
        last = recvs[r].shape[1] - 1
        row = jnp.sum(recvs[r][:, last, :], axis=0, keepdims=True)
        b = jnp.broadcast_to(row, (8, LANES))
        t = jnp.where(
            sub8 == 0, b, jnp.where(sub8 == 1, pltpu.roll(b, LANES - 16, 1), pltpu.roll(b, LANES - 32, 1))
        )
        return [jnp.broadcast_to(t[:, q : q + 1], (8, LANES)) for q in range(8)]

    send3[...] = jnp.zeros((8, LANES), jnp.float32)
    start_round(0)

    for c in range(C):
        for s in range(sub):
            line = jnp.broadcast_to(own_ref[c * sub + s : c * sub + s + 1, :], (LANES, LANES))
            rowb[c, s * LANES : (s + 1) * LANES, :] = line.T

    sums = wait_round(0)
    beta = jnp.sqrt(sums[3] + tiny)
    inv_beta = 1.0 / beta
    tails = [[jnp.zeros((8, LANES), jnp.float32)] * 4]
    moments = [[sums[4 + j] * inv_beta for j in range(4)]]
    scale0 = rows16(inv_beta)

    def slot_of(j):
        d = j // n_grp - wide
        place = blk + d
        valid = jnp.logical_and(place >= 0, place < n_blk)
        return lax.rem(n_blk - d, n_blk) * n_grp + j % n_grp, valid

    def fill(j, carry):
        slot, valid = slot_of(j)
        keep = jnp.where(valid, 1.0, 0.0).astype(jnp.float32)
        ccols[j] = recv0[slot, 0:16]
        v0[j] = recv0[slot, 16:32] * (scale0 * keep)
        return carry

    lax.fori_loop(0, near, fill, 0)

    ones8 = jnp.ones((8, LANES), jnp.float32)

    def lane_sums(c, s):
        tile = accb[c, s * LANES : (s + 1) * LANES, :]
        return lax.dot_general(
            ones8, tile, (((1,), (1,)), ((), ())),
            precision=lax.Precision.HIGHEST, preferred_element_type=jnp.float32,
        )[0:1]

    inner = (2 * REACH + 1) * n_grp

    def apply(values, first):
        def group(rg, carry):
            at = pl.ds(pl.multiple_of(rg * GROUP, GROUP), GROUP)
            if first:
                rx, ry, rz = rowb[0, at, :], rowb[1, at, :], rowb[2, at, :]

            def step(j, acc):
                acc = list(acc)
                jn = j + n_grp
                for s in range(sub):
                    if first:
                        dx = rx - ccols[jn, s : s + 1, :]
                        dy = ry - ccols[jn, sub + s : sub + s + 1, :]
                        dz = rz - ccols[jn, 2 * sub + s : 2 * sub + s + 1, :]
                        tile = jnp.exp2(-(dx * dx + dy * dy + dz * dz))
                        kbuf[j * sub + s, at, :] = tile
                    else:
                        tile = kbuf[j * sub + s, at, :]
                    for c in range(C):
                        acc[c] = acc[c] + tile * values[jn, c * sub + s : c * sub + s + 1, :]
                return tuple(acc)

            zero = jnp.zeros((GROUP, LANES), jnp.float32)
            acc = lax.fori_loop(0, inner, step, (zero,) * C)
            for c in range(C):
                accb[c, at, :] = acc[c]
            return carry

        lax.fori_loop(0, sub * LANES // GROUP, group, 0)

    hessenberg = []
    for k in range(ITERS):
        apply(heads[k], k == 0)
        image_tail = moments[k]
        block = sends[k + 1] if k + 1 < ITERS else wn.at[0]
        for c in range(C):
            for s in range(sub):
                line = lane_sums(c, s)
                if k > 0:
                    for j in range(4):
                        line = line + tails[k][j][c : c + 1] * p_own[j][s : s + 1]
                block[c * sub + s : c * sub + s + 1, :] = line
        row = dots_row(block[...], [heads[i][own_near] for i in range(k + 1)])
        last = sends[k + 1].shape[0] - 1
        sends[k + 1][last : last + 1, :] = row
        start_round(k + 1)
        if k + 1 == ITERS:
            for c in range(4):
                for s in range(tsub):
                    line = jnp.broadcast_to(tgt_ref[c * tsub + s : c * tsub + s + 1, :], (LANES, LANES))
                    rowb[c, s * LANES : (s + 1) * LANES, :] = line.T
        sums = wait_round(k + 1)
        full_sq = sums[3]
        for j in range(4):
            full_sq = full_sq + image_tail[j] * image_tail[j]
        rest_tail = list(image_tail)
        rest_moment = [sums[4 + j] for j in range(4)]
        column = []
        for i in range(k + 1):
            factor = sums[i]
            for j in range(4):
                factor = factor + tails[i][j] * image_tail[j]
            full_sq = full_sq - factor * factor
            for j in range(4):
                rest_tail[j] = rest_tail[j] - factor * tails[i][j]
                rest_moment[j] = rest_moment[j] - factor * moments[i][j]
            column.append(factor)
        length = jnp.sqrt(full_sq + tiny)
        inv_length = 1.0 / length
        hessenberg.append(column + [length])
        if k + 1 < ITERS:
            tails.append([t * inv_length for t in rest_tail])
            moments.append([m * inv_length for m in rest_moment])
            scale = rows16(inv_length)
            factors = [rows16(f * inv_length) for f in column]

            def advance(j, carry, k=k, scale=scale, factors=factors):
                slot, valid = slot_of(j)
                keep = jnp.where(valid, 1.0, 0.0).astype(jnp.float32)
                v = recvs[k + 1][slot] * (scale * keep)
                for i in range(k + 1):
                    v = v - factors[i] * heads[i][j]
                heads[k + 1][j] = v
                return carry

            lax.fori_loop(0, near, advance, 0)

    solved = least_squares(hessenberg, beta)
    poly = []
    for j in range(4):
        p = solved[0] * tails[0][j]
        for k in range(1, ITERS):
            p = p + solved[k] * tails[k][j]
        poly.append(p)
    lane8 = lax.broadcasted_iota(jnp.int32, (8, LANES), 1)
    packed = poly[3]
    for j in range(3):
        packed = jnp.where(lane8 == j, poly[j], packed)
    out_p[...] = packed
    spread = [rows16(y) for y in solved]

    def combine(j, carry):
        wn[j] = spread[0] * v0[j] + spread[1] * v1[j] + spread[2] * v2[j]
        return carry

    lax.fori_loop(0, near, combine, 0)
    out_w[...] = wn[own_near]

    def tgroup(rg, carry):
        at = pl.ds(pl.multiple_of(rg * GROUP, GROUP), GROUP)
        rx, ry, rz, own = rowb[0, at, :], rowb[1, at, :], rowb[2, at, :], rowb[3, at, :]
        zero = jnp.zeros((GROUP, LANES), jnp.float32)
        for c in range(C):
            accb[c, at, :] = zero

        def slab(d, carry2):
            def step(g, acc):
                acc = list(acc)
                jn = d * n_grp + g
                for s in range(sub):
                    dx = rx - ccols[jn, s : s + 1, :]
                    dy = ry - ccols[jn, sub + s : sub + s + 1, :]
                    dz = rz - ccols[jn, 2 * sub + s : 2 * sub + s + 1, :]
                    tile = jnp.exp2(-(dx * dx + dy * dy + dz * dz))
                    for c in range(C):
                        acc[c] = acc[c] + tile * wn[jn, c * sub + s : c * sub + s + 1, :]
                return tuple(acc)

            acc = lax.fori_loop(0, n_grp, step, (zero,) * C)
            away = (d - wide).astype(jnp.float32)
            hit = jnp.abs(own - away) <= REACH + 0.5
            for c in range(C):
                accb[c, at, :] = accb[c, at, :] + jnp.where(hit, acc[c], 0.0)
            return carry2

        lax.fori_loop(0, 2 * wide + 1, slab, 0)
        return carry

    lax.fori_loop(0, tsub * LANES // GROUP, tgroup, 0)
    for r in range(ITERS + 1):
        sent = recvs[r].at[pl.ds(1, peers - 1)]
        pltpu.make_async_copy(sent, sent, send_sem.at[r]).wait()
    q_own = basis_rows(tgt_ref[0:tsub], tgt_ref[tsub : 2 * tsub], tgt_ref[2 * tsub : 3 * tsub])
    out_m[...] = jnp.zeros((16, LANES), jnp.float32)
    for c in range(C):
        for s in range(tsub):
            line = lane_sums(c, s)
            for j in range(4):
                line = line + poly[j][c : c + 1] * q_own[j][s : s + 1]
            out_m[c * tsub + s : c * tsub + s + 1, :] = line


def shards(source_coords, source_values, target_coords, target_owner):
    own_rows = source_coords.shape[1]
    own_tgt = target_coords.shape[1]
    n_grp = lax.axis_size("grp")
    n_blk = lax.axis_size("blk")
    sub = own_rows // LANES
    tsub = own_tgt // LANES
    slab_len = own_rows * n_grp
    root_n = math.sqrt(slab_len * n_blk)
    log2e = 1.0 / math.log(2.0)
    scale_x = math.sqrt(thin_factor * log2e)
    scale_y = math.sqrt(4.0 * slab_len * log2e)
    blk = lax.axis_index("blk")
    scales = jnp.array([[scale_x], [scale_y], [scale_y]], jnp.float32)
    shift = jnp.array([[0.0], [0.5], [0.5]], jnp.float32)
    pad = jnp.zeros((1, LANES), jnp.float32)
    own = jnp.concatenate(
        [
            ((source_coords - shift) * scales).reshape(3 * sub, LANES),
            pad,
            source_values.reshape(3 * sub, LANES),
            pad,
        ]
    )
    tgt = jnp.concatenate(
        [
            ((target_coords - shift) * scales).reshape(3 * tsub, LANES),
            (target_owner - blk).astype(jnp.float32).reshape(tsub, LANES),
        ]
    )
    peers = n_blk * n_grp
    near = (2 * REACH + 3) * n_grp
    inner = (2 * REACH + 1) * n_grp
    f32 = jnp.float32
    vmem = pl.BlockSpec(memory_space=pltpu.VMEM)
    out_w, out_m, out_p = pl.pallas_call(
        functools.partial(kernel, n_blk, n_grp, sub, tsub, scale_x, scale_y, root_n),
        out_shape=(
            jax.ShapeDtypeStruct((16, LANES), f32),
            jax.ShapeDtypeStruct((16, LANES), f32),
            jax.ShapeDtypeStruct((8, LANES), f32),
        ),
        in_specs=[vmem, vmem],
        out_specs=(vmem, vmem, vmem),
        scratch_shapes=[
            pltpu.VMEM((inner * sub, own_rows, LANES), f32),
            pltpu.VMEM((4, own_rows, LANES), f32),
            pltpu.VMEM((C, own_rows, LANES), f32),
            pltpu.VMEM((peers, 32, LANES), f32),
            pltpu.VMEM((peers, 16, LANES), f32),
            pltpu.VMEM((peers, 16, LANES), f32),
            pltpu.VMEM((peers, 8, LANES), f32),
            pltpu.VMEM((32, LANES), f32),
            pltpu.VMEM((16, LANES), f32),
            pltpu.VMEM((16, LANES), f32),
            pltpu.VMEM((8, LANES), f32),
            pltpu.VMEM((near, 16, LANES), f32),
            pltpu.VMEM((near, 16, LANES), f32),
            pltpu.VMEM((near, 16, LANES), f32),
            pltpu.VMEM((near, 16, LANES), f32),
            pltpu.VMEM((near, 16, LANES), f32),
            pltpu.SemaphoreType.DMA((4,)),
            pltpu.SemaphoreType.DMA((4,)),
        ],
        compiler_params=pltpu.CompilerParams(
            collective_id=0, has_side_effects=True, vmem_limit_bytes=60 * 1024 * 1024
        ),
    )(own, tgt)
    weights = out_w[: C * sub].reshape(C, own_rows)
    mapped = out_m[: C * tsub].reshape(C, own_tgt)
    return weights, out_p[:C, :4], mapped


def solution(mesh):
    return jax.shard_map(
        shards,
        mesh=mesh,
        in_specs=(
            P(None, ("blk", "grp")),
            P(None, ("blk", "grp")),
            P(None, ("blk", "grp")),
            P(("blk", "grp")),
        ),
        out_specs=(P(None, ("blk", "grp")), P(), P(None, ("blk", "grp"))),
        check_vma=False,
    )
```

```python
import functools
import math

import jax
import jax.numpy as jnp
from jax import lax
from jax.experimental import pallas as pl
from jax.experimental.pallas import tpu as pltpu
from jax.sharding import PartitionSpec as P

ITERS = 3
REACH = 2
C = 3
thin_factor = 0.6
tiny = 1e-06
LANES = 128
GROUP = 64
HELD = 3
MESH = pl.DeviceIdType.MESH


def least_squares(hessenberg, beta):
    count = len(hessenberg)
    right_side = [beta] + [jnp.zeros_like(beta) for k in range(count)]
    upper, cosines, sines = [], [], []
    for k in range(count):
        column = list(hessenberg[k])
        for i in range(k):
            top = cosines[i] * column[i] + sines[i] * column[i + 1]
            lower = -sines[i] * column[i] + cosines[i] * column[i + 1]
            column[i] = top
            column[i + 1] = lower
        radius = jnp.sqrt(column[k] * column[k] + column[k + 1] * column[k + 1])
        cosine = column[k] / radius
        sine = column[k + 1] / radius
        column[k] = radius
        cosines.append(cosine)
        sines.append(sine)
        right_side[k + 1] = -sine * right_side[k]
        right_side[k] = cosine * right_side[k]
        upper.append(column[: k + 1])
    solved = [None] * count
    for k in reversed(range(count)):
        running = right_side[k]
        for j in range(k + 1, count):
            running = running - upper[j][k] * solved[j]
        solved[k] = running / upper[k][k]
    return solved


def kernel(
    n_blk, n_grp, sub, tsub, scale_x, scale_y, root_n,
    own_ref, tgt_ref, out_w, out_m, out_p,
    kbuf, fbuf, rowb, trowb, accb, recv0, recv1, recv2, recv3, send0, send1, send2, send3,
    ccols, v0, v1, v2, wn, send_sem, recv_sem,
):
    blk = lax.axis_index("blk")
    grp = lax.axis_index("grp")
    peers = n_blk * n_grp
    wide = REACH + 1
    near = (2 * wide + 1) * n_grp
    recvs = (recv0, recv1, recv2, recv3)
    sends = (send0, send1, send2, send3)
    heads = (v0, v1, v2)
    own_near = wide * n_grp

    def target(p):
        e = p // n_grp
        h = p % n_grp
        return lax.rem(blk + e, n_blk), lax.rem(grp + h, n_grp), e

    barrier = pltpu.get_barrier_semaphore()

    def greet(p, carry):
        tb, tg, e = target(p)
        pl.semaphore_signal(barrier, inc=1, device_id=(tb, tg), device_id_type=MESH)
        return carry

    lax.fori_loop(1, peers, greet, 0)

    lane = lax.broadcasted_iota(jnp.int32, (1, LANES), 1)
    sub8 = lax.broadcasted_iota(jnp.int32, (8, LANES), 0)
    sub16 = lax.broadcasted_iota(jnp.int32, (16, LANES), 0)

    def rows16(f):
        return jnp.where(sub16 < sub, f[0:1], jnp.where(sub16 < 2 * sub, f[1:2], f[2:3]))

    x_own = own_ref[0:sub]
    y_own = own_ref[sub : 2 * sub]
    z_own = own_ref[2 * sub : 3 * sub]

    def basis_rows(x, y, z):
        return (
            jnp.full_like(x, 1.0 / root_n),
            (x * (2.0 / (n_blk * scale_x)) - 1.0) * (1.0 / root_n),
            y * (2.0 / (scale_y * root_n)),
            z * (2.0 / (scale_y * root_n)),
        )

    p_own = basis_rows(x_own, y_own, z_own)

    def total(a):
        return jnp.sum(jnp.sum(a, axis=0, keepdims=True), axis=1, keepdims=True)

    def dots_row(w, others):
        row = jnp.zeros((1, LANES), jnp.float32)
        for c in range(C):
            wc = w[c * sub : (c + 1) * sub]
            terms = [(i, total(wc * o[c * sub : (c + 1) * sub])) for i, o in enumerate(others)]
            terms.append((3, total(wc * wc)))
            terms += [(4 + j, total(wc * p_own[j])) for j in range(4)]
            for q, value in terms:
                row = jnp.where(lane == 16 * c + q, value, row)
        return row

    vals = own_ref[16:32]
    row0 = dots_row(vals, [])
    send0[0:16] = own_ref[0:16]
    send0[16:31] = own_ref[16:31]
    send0[31:32] = row0
    pl.semaphore_wait(barrier, peers - 1)

    def copy_to(r, p):
        tb, tg, e = target(p)
        return pltpu.make_async_remote_copy(
            src_ref=sends[r],
            dst_ref=recvs[r].at[p],
            send_sem=send_sem.at[r],
            recv_sem=recv_sem.at[r],
            device_id=(tb, tg),
            device_id_type=MESH,
        )

    def start_round(r):
        def body(p, carry):
            copy_to(r, p).start()
            return carry

        lax.fori_loop(1, peers, body, 0)
        recvs[r][0] = sends[r][...]

    def wait_round(r):
        landed = recvs[r].at[pl.ds(1, peers - 1)]
        pltpu.make_async_copy(landed, landed, recv_sem.at[r]).wait()
        last = recvs[r].shape[1] - 1
        row = jnp.sum(recvs[r][:, last, :], axis=0, keepdims=True)
        b = jnp.broadcast_to(row, (8, LANES))
        t = jnp.where(
            sub8 == 0, b, jnp.where(sub8 == 1, pltpu.roll(b, LANES - 16, 1), pltpu.roll(b, LANES - 32, 1))
        )
        return [jnp.broadcast_to(t[:, q : q + 1], (8, LANES)) for q in range(8)]

    start_round(0)

    for c in range(C):
        for s in range(sub):
            line = jnp.broadcast_to(own_ref[c * sub + s : c * sub + s + 1, :], (LANES, LANES))
            rowb[c, s * LANES : (s + 1) * LANES, :] = line.T

    for c in range(4):
        for s in range(tsub):
            line = jnp.broadcast_to(tgt_ref[c * tsub + s : c * tsub + s + 1, :], (LANES, LANES))
            trowb[c, s * LANES : (s + 1) * LANES, :] = line.T

    sums = wait_round(0)
    beta = jnp.sqrt(sums[3] + tiny)
    inv_beta = 1.0 / beta
    tails = [[jnp.zeros((8, LANES), jnp.float32)] * 4]
    moments = [[sums[4 + j] * inv_beta for j in range(4)]]
    scale0 = rows16(inv_beta)

    def slot_of(j):
        d = j // n_grp - wide
        place = blk + d
        valid = jnp.logical_and(place >= 0, place < n_blk)
        return lax.rem(n_blk - d, n_blk) * n_grp + j % n_grp, valid

    def fill(j, carry):
        slot, valid = slot_of(j)
        keep = jnp.where(valid, 1.0, 0.0).astype(jnp.float32)
        ccols[j] = recv0[slot, 0:16]
        v0[j] = recv0[slot, 16:32] * (scale0 * keep)
        return carry

    lax.fori_loop(0, near, fill, 0)

    ones8 = jnp.ones((8, LANES), jnp.float32)

    def lane_sums(c, s):
        tile = accb[c, s * LANES : (s + 1) * LANES, :]
        return jnp.sum(tile.T, axis=0, keepdims=True)

    inner = (2 * REACH + 1) * n_grp

    def apply(values, first):
        def group(rg, carry):
            at = pl.ds(pl.multiple_of(rg * GROUP, GROUP), GROUP)
            if first:
                rx, ry, rz = rowb[0, at, :], rowb[1, at, :], rowb[2, at, :]

            def step(j, acc):
                acc = list(acc)
                jn = j + n_grp
                for s in range(sub):
                    if first:
                        dx = rx - ccols[jn, s : s + 1, :]
                        dy = ry - ccols[jn, sub + s : sub + s + 1, :]
                        dz = rz - ccols[jn, 2 * sub + s : 2 * sub + s + 1, :]
                        tile = jnp.exp2(-(dx * dx + dy * dy + dz * dz))
                        kbuf[j * sub + s, at, :] = tile
                    else:
                        tile = kbuf[j * sub + s, at, :]
                    for c in range(C):
                        acc[c] = acc[c] + tile * values[jn, c * sub + s : c * sub + s + 1, :]
                return tuple(acc)

            zero = jnp.zeros((GROUP, LANES), jnp.float32)
            acc = lax.fori_loop(0, inner, step, (zero,) * C)
            for c in range(C):
                accb[c, at, :] = acc[c]
            return carry

        lax.fori_loop(0, sub * LANES // GROUP, group, 0)

    def make_tiles(buf, base, low, high):
        def group(rg, carry):
            at = pl.ds(pl.multiple_of(rg * GROUP, GROUP), GROUP)
            rx, ry, rz = trowb[0, at, :], trowb[1, at, :], trowb[2, at, :]

            def step(jn, carry2):
                for s in range(sub):
                    dx = rx - ccols[jn, s : s + 1, :]
                    dy = ry - ccols[jn, sub + s : sub + s + 1, :]
                    dz = rz - ccols[jn, 2 * sub + s : 2 * sub + s + 1, :]
                    tile = jnp.exp2(-(dx * dx + dy * dy + dz * dz))
                    buf[(jn - base * n_grp) * sub + s, at, :] = tile
                return carry2

            return lax.fori_loop(low * n_grp, high * n_grp, step, carry)

        lax.fori_loop(0, tsub * LANES // GROUP, group, 0)

    hessenberg = []
    for k in range(ITERS):
        apply(heads[k], k == 0)
        image_tail = moments[k]
        block = sends[k + 1] if k + 1 < ITERS else wn.at[0]
        for c in range(C):
            for s in range(sub):
                line = lane_sums(c, s)
                if k > 0:
                    for j in range(4):
                        line = line + tails[k][j][c : c + 1] * p_own[j][s : s + 1]
                block[c * sub + s : c * sub + s + 1, :] = line
        row = dots_row(block[...], [heads[i][own_near] for i in range(k + 1)])
        last = sends[k + 1].shape[0] - 1
        sends[k + 1][last : last + 1, :] = row
        start_round(k + 1)
        if k == 0:
            make_tiles(fbuf, 0, 0, 2)
        elif k == 1:
            make_tiles(fbuf, 0, 2, HELD)
        elif k + 1 == ITERS:
            make_tiles(kbuf, HELD, HELD, 2 * wide + 1)
        sums = wait_round(k + 1)
        full_sq = sums[3]
        for j in range(4):
            full_sq = full_sq + image_tail[j] * image_tail[j]
        rest_tail = list(image_tail)
        rest_moment = [sums[4 + j] for j in range(4)]
        column = []
        for i in range(k + 1):
            factor = sums[i]
            for j in range(4):
                factor = factor + tails[i][j] * image_tail[j]
            full_sq = full_sq - factor * factor
            for j in range(4):
                rest_tail[j] = rest_tail[j] - factor * tails[i][j]
                rest_moment[j] = rest_moment[j] - factor * moments[i][j]
            column.append(factor)
        length = jnp.sqrt(full_sq + tiny)
        inv_length = 1.0 / length
        hessenberg.append(column + [length])
        if k + 1 < ITERS:
            tails.append([t * inv_length for t in rest_tail])
            moments.append([m * inv_length for m in rest_moment])
            scale = rows16(inv_length)
            factors = [rows16(f * inv_length) for f in column]

            def advance(j, carry, k=k, scale=scale, factors=factors):
                slot, valid = slot_of(j)
                keep = jnp.where(valid, 1.0, 0.0).astype(jnp.float32)
                v = recvs[k + 1][slot] * (scale * keep)
                for i in range(k + 1):
                    v = v - factors[i] * heads[i][j]
                heads[k + 1][j] = v
                return carry

            lax.fori_loop(0, near, advance, 0)

    solved = least_squares(hessenberg, beta)
    poly = []
    for j in range(4):
        p = solved[0] * tails[0][j]
        for k in range(1, ITERS):
            p = p + solved[k] * tails[k][j]
        poly.append(p)
    lane8 = lax.broadcasted_iota(jnp.int32, (8, LANES), 1)
    packed = poly[3]
    for j in range(3):
        packed = jnp.where(lane8 == j, poly[j], packed)
    out_p[...] = packed
    spread = [rows16(y) for y in solved]

    def combine(j, carry):
        wn[j] = spread[0] * v0[j] + spread[1] * v1[j] + spread[2] * v2[j]
        return carry

    lax.fori_loop(0, near, combine, 0)
    out_w[...] = wn[own_near]

    def tgroup(rg, carry):
        at = pl.ds(pl.multiple_of(rg * GROUP, GROUP), GROUP)
        own = trowb[3, at, :]
        zero = jnp.zeros((GROUP, LANES), jnp.float32)
        for c in range(C):
            accb[c, at, :] = zero

        def slabs_of(buf, base, low, high):
            def slab(d, carry2):
                def step(g, acc):
                    acc = list(acc)
                    jn = d * n_grp + g
                    for s in range(sub):
                        tile = buf[(jn - base * n_grp) * sub + s, at, :]
                        for c in range(C):
                            acc[c] = acc[c] + tile * wn[jn, c * sub + s : c * sub + s + 1, :]
                    return tuple(acc)

                acc = lax.fori_loop(0, n_grp, step, (zero,) * C)
                away = (d - wide).astype(jnp.float32)
                hit = jnp.abs(own - away) <= REACH + 0.5
                for c in range(C):
                    accb[c, at, :] = accb[c, at, :] + jnp.where(hit, acc[c], 0.0)
                return carry2

            lax.fori_loop(low, high, slab, 0)

        slabs_of(fbuf, 0, 0, HELD)
        slabs_of(kbuf, HELD, HELD, 2 * wide + 1)
        return carry

    lax.fori_loop(0, tsub * LANES // GROUP, tgroup, 0)
    for r in range(ITERS + 1):
        sent = recvs[r].at[pl.ds(1, peers - 1)]
        pltpu.make_async_copy(sent, sent, send_sem.at[r]).wait()
    q_own = basis_rows(tgt_ref[0:tsub], tgt_ref[tsub : 2 * tsub], tgt_ref[2 * tsub : 3 * tsub])
    out_m[...] = jnp.zeros((16, LANES), jnp.float32)
    for c in range(C):
        for s in range(tsub):
            line = lane_sums(c, s)
            for j in range(4):
                line = line + poly[j][c : c + 1] * q_own[j][s : s + 1]
            out_m[c * tsub + s : c * tsub + s + 1, :] = line


def shards(source_coords, source_values, target_coords, target_owner):
    own_rows = source_coords.shape[1]
    own_tgt = target_coords.shape[1]
    n_grp = lax.axis_size("grp")
    n_blk = lax.axis_size("blk")
    sub = own_rows // LANES
    tsub = own_tgt // LANES
    slab_len = own_rows * n_grp
    root_n = math.sqrt(slab_len * n_blk)
    log2e = 1.0 / math.log(2.0)
    scale_x = math.sqrt(thin_factor * log2e)
    scale_y = math.sqrt(4.0 * slab_len * log2e)
    blk = lax.axis_index("blk")
    scales = jnp.array([[scale_x], [scale_y], [scale_y]], jnp.float32)
    shift = jnp.array([[0.0], [0.5], [0.5]], jnp.float32)
    pad = jnp.zeros((1, LANES), jnp.float32)
    own = jnp.concatenate(
        [
            ((source_coords - shift) * scales).reshape(3 * sub, LANES),
            pad,
            source_values.reshape(3 * sub, LANES),
            pad,
        ]
    )
    tgt = jnp.concatenate(
        [
            ((target_coords - shift) * scales).reshape(3 * tsub, LANES),
            (target_owner - blk).astype(jnp.float32).reshape(tsub, LANES),
        ]
    )
    peers = n_blk * n_grp
    near = (2 * REACH + 3) * n_grp
    inner = (2 * REACH + 1) * n_grp
    f32 = jnp.float32
    vmem = pl.BlockSpec(memory_space=pltpu.VMEM)
    out_w, out_m, out_p = pl.pallas_call(
        functools.partial(kernel, n_blk, n_grp, sub, tsub, scale_x, scale_y, root_n),
        out_shape=(
            jax.ShapeDtypeStruct((16, LANES), f32),
            jax.ShapeDtypeStruct((16, LANES), f32),
            jax.ShapeDtypeStruct((8, LANES), f32),
        ),
        in_specs=[vmem, vmem],
        out_specs=(vmem, vmem, vmem),
        scratch_shapes=[
            pltpu.VMEM((inner * sub, own_rows, LANES), f32),
            pltpu.VMEM((HELD * n_grp * sub, own_tgt, LANES), f32),
            pltpu.VMEM((3, own_rows, LANES), f32),
            pltpu.VMEM((4, own_tgt, LANES), f32),
            pltpu.VMEM((C, own_rows, LANES), f32),
            pltpu.VMEM((peers, 32, LANES), f32),
            pltpu.VMEM((peers, 16, LANES), f32),
            pltpu.VMEM((peers, 16, LANES), f32),
            pltpu.VMEM((peers, 1, LANES), f32),
            pltpu.VMEM((32, LANES), f32),
            pltpu.VMEM((16, LANES), f32),
            pltpu.VMEM((16, LANES), f32),
            pltpu.VMEM((1, LANES), f32),
            pltpu.VMEM((near, 16, LANES), f32),
            pltpu.VMEM((near, 16, LANES), f32),
            pltpu.VMEM((near, 16, LANES), f32),
            pltpu.VMEM((near, 16, LANES), f32),
            pltpu.VMEM((near, 16, LANES), f32),
            pltpu.SemaphoreType.DMA((4,)),
            pltpu.SemaphoreType.DMA((4,)),
        ],
        compiler_params=pltpu.CompilerParams(
            collective_id=0, has_side_effects=True, vmem_limit_bytes=63 * 1024 * 1024
        ),
    )(own, tgt)
    weights = out_w[: C * sub].reshape(C, own_rows)
    mapped = out_m[: C * tsub].reshape(C, own_tgt)
    return weights, out_p[:C, :4], mapped


def solution(mesh):
    return jax.shard_map(
        shards,
        mesh=mesh,
        in_specs=(
            P(None, ("blk", "grp")),
            P(None, ("blk", "grp")),
            P(None, ("blk", "grp")),
            P(("blk", "grp")),
        ),
        out_specs=(P(None, ("blk", "grp")), P(), P(None, ("blk", "grp"))),
        check_vma=False,
    )
```

```python
import functools
import math

import jax
import jax.numpy as jnp
from jax import lax
from jax.experimental import pallas as pl
from jax.experimental.pallas import tpu as pltpu
from jax.sharding import PartitionSpec as P

ITERS = 3
REACH = 2
C = 3
thin_factor = 0.6
tiny = 1e-06
LANES = 128
GROUP = 64
HELD = 3
MESH = pl.DeviceIdType.MESH


def least_squares(hessenberg, beta):
    count = len(hessenberg)
    right_side = [beta] + [jnp.zeros_like(beta) for k in range(count)]
    upper, cosines, sines = [], [], []
    for k in range(count):
        column = list(hessenberg[k])
        for i in range(k):
            top = cosines[i] * column[i] + sines[i] * column[i + 1]
            lower = -sines[i] * column[i] + cosines[i] * column[i + 1]
            column[i] = top
            column[i + 1] = lower
        radius = jnp.sqrt(column[k] * column[k] + column[k + 1] * column[k + 1])
        cosine = column[k] / radius
        sine = column[k + 1] / radius
        column[k] = radius
        cosines.append(cosine)
        sines.append(sine)
        right_side[k + 1] = -sine * right_side[k]
        right_side[k] = cosine * right_side[k]
        upper.append(column[: k + 1])
    solved = [None] * count
    for k in reversed(range(count)):
        running = right_side[k]
        for j in range(k + 1, count):
            running = running - upper[j][k] * solved[j]
        solved[k] = running / upper[k][k]
    return solved


def kernel(
    n_blk, n_grp, sub, tsub, scale_x, scale_y, root_n,
    own_ref, tgt_ref, out_w, out_m, out_p,
    kbuf, fbuf, rowb, trowb, accb, recv0, recv1, recv2, recv3, send0, send1, send2, send3,
    ccols, v0, v1, v2, wn, send_sem, recv_sem,
):
    blk = lax.axis_index("blk")
    grp = lax.axis_index("grp")
    peers = n_blk * n_grp
    wide = REACH + 1
    near = (2 * wide + 1) * n_grp
    recvs = (recv0, recv1, recv2, recv3)
    sends = (send0, send1, send2, send3)
    heads = (v0, v1, v2)
    own_near = wide * n_grp

    def target(p):
        e = p // n_grp
        h = p % n_grp
        return lax.rem(blk + e, n_blk), lax.rem(grp + h, n_grp), e

    barrier = pltpu.get_barrier_semaphore()

    def greet(p, carry):
        tb, tg, e = target(p)
        pl.semaphore_signal(barrier, inc=1, device_id=(tb, tg), device_id_type=MESH)
        return carry

    lax.fori_loop(1, peers, greet, 0)

    lane = lax.broadcasted_iota(jnp.int32, (1, LANES), 1)
    sub8 = lax.broadcasted_iota(jnp.int32, (8, LANES), 0)
    sub16 = lax.broadcasted_iota(jnp.int32, (16, LANES), 0)

    def rows16(f):
        return jnp.where(sub16 < sub, f[0:1], jnp.where(sub16 < 2 * sub, f[1:2], f[2:3]))

    x_own = own_ref[0:sub]
    y_own = own_ref[sub : 2 * sub]
    z_own = own_ref[2 * sub : 3 * sub]

    def basis_rows(x, y, z):
        return (
            jnp.full_like(x, 1.0 / root_n),
            (x * (2.0 / (n_blk * scale_x)) - 1.0) * (1.0 / root_n),
            y * (2.0 / (scale_y * root_n)),
            z * (2.0 / (scale_y * root_n)),
        )

    p_own = basis_rows(x_own, y_own, z_own)

    def total(a):
        return jnp.sum(jnp.sum(a, axis=0, keepdims=True), axis=1, keepdims=True)

    def dots_row(w, others):
        row = jnp.zeros((1, LANES), jnp.float32)
        for c in range(C):
            wc = w[c * sub : (c + 1) * sub]
            terms = [(i, total(wc * o[c * sub : (c + 1) * sub])) for i, o in enumerate(others)]
            terms.append((3, total(wc * wc)))
            terms += [(4 + j, total(wc * p_own[j])) for j in range(4)]
            for q, value in terms:
                row = jnp.where(lane == 16 * c + q, value, row)
        return row

    vals = own_ref[16:32]
    row0 = dots_row(vals, [])
    send0[0:16] = own_ref[0:16]
    send0[16:31] = own_ref[16:31]
    send0[31:32] = row0
    pl.semaphore_wait(barrier, peers - 1)

    far_low, far_high = (wide + 1) * n_grp, (n_blk - wide) * n_grp
    parts = ((1, far_low, False), (far_low, far_high, True), (far_high, peers, False))

    def rows_of(r, far):
        rows = recvs[r].shape[1]
        count = min(8, rows) if far else rows
        return pl.ds(rows - count, count)

    def start_round(r):
        for part, (low, high, far) in enumerate(parts):
            rows = rows_of(r, far)

            def body(p, carry, part=part, rows=rows):
                tb, tg, e = target(p)
                pltpu.make_async_remote_copy(
                    src_ref=sends[r].at[rows],
                    dst_ref=recvs[r].at[p, rows],
                    send_sem=send_sem.at[r, part],
                    recv_sem=recv_sem.at[r, part],
                    device_id=(tb, tg),
                    device_id_type=MESH,
                ).start()
                return carry

            lax.fori_loop(low, high, body, 0)
        recvs[r][0] = sends[r][...]

    def wait_bytes(r, sem):
        for part, (low, high, far) in enumerate(parts):
            if high > low:
                landed = recvs[r].at[pl.ds(low, high - low), rows_of(r, far)]
                pltpu.make_async_copy(landed, landed, sem.at[r, part]).wait()

    def wait_round(r):
        wait_bytes(r, recv_sem)
        last = recvs[r].shape[1] - 1
        row = jnp.sum(recvs[r][:, last, :], axis=0, keepdims=True)
        b = jnp.broadcast_to(row, (8, LANES))
        t = jnp.where(
            sub8 == 0, b, jnp.where(sub8 == 1, pltpu.roll(b, LANES - 16, 1), pltpu.roll(b, LANES - 32, 1))
        )
        return [jnp.broadcast_to(t[:, q : q + 1], (8, LANES)) for q in range(8)]

    start_round(0)

    for c in range(C):
        for s in range(sub):
            line = jnp.broadcast_to(own_ref[c * sub + s : c * sub + s + 1, :], (LANES, LANES))
            rowb[c, s * LANES : (s + 1) * LANES, :] = line.T

    for c in range(4):
        for s in range(tsub):
            line = jnp.broadcast_to(tgt_ref[c * tsub + s : c * tsub + s + 1, :], (LANES, LANES))
            trowb[c, s * LANES : (s + 1) * LANES, :] = line.T

    sums = wait_round(0)
    beta = jnp.sqrt(sums[3] + tiny)
    inv_beta = 1.0 / beta
    tails = [[jnp.zeros((8, LANES), jnp.float32)] * 4]
    moments = [[sums[4 + j] * inv_beta for j in range(4)]]
    scale0 = rows16(inv_beta)

    def slot_of(j):
        d = j // n_grp - wide
        place = blk + d
        valid = jnp.logical_and(place >= 0, place < n_blk)
        return lax.rem(n_blk - d, n_blk) * n_grp + j % n_grp, valid

    def fill(j, carry):
        slot, valid = slot_of(j)
        keep = jnp.where(valid, 1.0, 0.0).astype(jnp.float32)
        ccols[j] = recv0[slot, 0:16]
        v0[j] = recv0[slot, 16:32] * (scale0 * keep)
        return carry

    lax.fori_loop(0, near, fill, 0)

    ones8 = jnp.ones((8, LANES), jnp.float32)

    def lane_sums(c, s):
        tile = accb[c, s * LANES : (s + 1) * LANES, :]
        return jnp.sum(tile.T, axis=0, keepdims=True)

    inner = (2 * REACH + 1) * n_grp

    def apply(values, first):
        def group(rg, carry):
            at = pl.ds(pl.multiple_of(rg * GROUP, GROUP), GROUP)
            if first:
                rx, ry, rz = rowb[0, at, :], rowb[1, at, :], rowb[2, at, :]

            def step(j, acc):
                acc = list(acc)
                jn = j + n_grp
                for s in range(sub):
                    if first:
                        dx = rx - ccols[jn, s : s + 1, :]
                        dy = ry - ccols[jn, sub + s : sub + s + 1, :]
                        dz = rz - ccols[jn, 2 * sub + s : 2 * sub + s + 1, :]
                        tile = jnp.exp2(-(dx * dx + dy * dy + dz * dz))
                        kbuf[j * sub + s, at, :] = tile
                    else:
                        tile = kbuf[j * sub + s, at, :]
                    for c in range(C):
                        acc[c] = acc[c] + tile * values[jn, c * sub + s : c * sub + s + 1, :]
                return tuple(acc)

            zero = jnp.zeros((GROUP, LANES), jnp.float32)
            acc = lax.fori_loop(0, inner, step, (zero,) * C)
            for c in range(C):
                accb[c, at, :] = acc[c]
            return carry

        lax.fori_loop(0, sub * LANES // GROUP, group, 0)

    def make_tiles(buf, base, low, high):
        def group(rg, carry):
            at = pl.ds(pl.multiple_of(rg * GROUP, GROUP), GROUP)
            rx, ry, rz = trowb[0, at, :], trowb[1, at, :], trowb[2, at, :]

            def step(jn, carry2):
                for s in range(sub):
                    dx = rx - ccols[jn, s : s + 1, :]
                    dy = ry - ccols[jn, sub + s : sub + s + 1, :]
                    dz = rz - ccols[jn, 2 * sub + s : 2 * sub + s + 1, :]
                    tile = jnp.exp2(-(dx * dx + dy * dy + dz * dz))
                    buf[(jn - base * n_grp) * sub + s, at, :] = tile
                return carry2

            return lax.fori_loop(low * n_grp, high * n_grp, step, carry)

        lax.fori_loop(0, tsub * LANES // GROUP, group, 0)

    hessenberg = []
    for k in range(ITERS):
        apply(heads[k], k == 0)
        image_tail = moments[k]
        block = sends[k + 1] if k + 1 < ITERS else wn.at[0]
        for c in range(C):
            for s in range(sub):
                line = lane_sums(c, s)
                if k > 0:
                    for j in range(4):
                        line = line + tails[k][j][c : c + 1] * p_own[j][s : s + 1]
                block[c * sub + s : c * sub + s + 1, :] = line
        row = dots_row(block[...], [heads[i][own_near] for i in range(k + 1)])
        last = sends[k + 1].shape[0] - 1
        sends[k + 1][last : last + 1, :] = row
        start_round(k + 1)
        if k == 0:
            make_tiles(fbuf, 0, 0, 2)
        elif k == 1:
            make_tiles(fbuf, 0, 2, HELD)
        elif k + 1 == ITERS:
            make_tiles(kbuf, HELD, HELD, 2 * wide + 1)
        sums = wait_round(k + 1)
        full_sq = sums[3]
        for j in range(4):
            full_sq = full_sq + image_tail[j] * image_tail[j]
        rest_tail = list(image_tail)
        rest_moment = [sums[4 + j] for j in range(4)]
        column = []
        for i in range(k + 1):
            factor = sums[i]
            for j in range(4):
                factor = factor + tails[i][j] * image_tail[j]
            full_sq = full_sq - factor * factor
            for j in range(4):
                rest_tail[j] = rest_tail[j] - factor * tails[i][j]
                rest_moment[j] = rest_moment[j] - factor * moments[i][j]
            column.append(factor)
        length = jnp.sqrt(full_sq + tiny)
        inv_length = 1.0 / length
        hessenberg.append(column + [length])
        if k + 1 < ITERS:
            tails.append([t * inv_length for t in rest_tail])
            moments.append([m * inv_length for m in rest_moment])
            scale = rows16(inv_length)
            factors = [rows16(f * inv_length) for f in column]

            def advance(j, carry, k=k, scale=scale, factors=factors):
                slot, valid = slot_of(j)
                keep = jnp.where(valid, 1.0, 0.0).astype(jnp.float32)
                v = recvs[k + 1][slot] * (scale * keep)
                for i in range(k + 1):
                    v = v - factors[i] * heads[i][j]
                heads[k + 1][j] = v
                return carry

            lax.fori_loop(0, near, advance, 0)

    solved = least_squares(hessenberg, beta)
    poly = []
    for j in range(4):
        p = solved[0] * tails[0][j]
        for k in range(1, ITERS):
            p = p + solved[k] * tails[k][j]
        poly.append(p)
    lane8 = lax.broadcasted_iota(jnp.int32, (8, LANES), 1)
    packed = poly[3]
    for j in range(3):
        packed = jnp.where(lane8 == j, poly[j], packed)
    out_p[...] = packed
    spread = [rows16(y) for y in solved]

    def combine(j, carry):
        wn[j] = spread[0] * v0[j] + spread[1] * v1[j] + spread[2] * v2[j]
        return carry

    lax.fori_loop(0, near, combine, 0)
    out_w[...] = wn[own_near]

    def tgroup(rg, carry):
        at = pl.ds(pl.multiple_of(rg * GROUP, GROUP), GROUP)
        own = trowb[3, at, :]
        zero = jnp.zeros((GROUP, LANES), jnp.float32)
        for c in range(C):
            accb[c, at, :] = zero

        def slabs_of(buf, base, low, high):
            def slab(d, carry2):
                def step(g, acc):
                    acc = list(acc)
                    jn = d * n_grp + g
                    for s in range(sub):
                        tile = buf[(jn - base * n_grp) * sub + s, at, :]
                        for c in range(C):
                            acc[c] = acc[c] + tile * wn[jn, c * sub + s : c * sub + s + 1, :]
                    return tuple(acc)

                acc = lax.fori_loop(0, n_grp, step, (zero,) * C)
                away = (d - wide).astype(jnp.float32)
                hit = jnp.abs(own - away) <= REACH + 0.5
                for c in range(C):
                    accb[c, at, :] = accb[c, at, :] + jnp.where(hit, acc[c], 0.0)
                return carry2

            lax.fori_loop(low, high, slab, 0)

        slabs_of(fbuf, 0, 0, HELD)
        slabs_of(kbuf, HELD, HELD, 2 * wide + 1)
        return carry

    lax.fori_loop(0, tsub * LANES // GROUP, tgroup, 0)
    for r in range(ITERS + 1):
        wait_bytes(r, send_sem)
    q_own = basis_rows(tgt_ref[0:tsub], tgt_ref[tsub : 2 * tsub], tgt_ref[2 * tsub : 3 * tsub])
    out_m[...] = jnp.zeros((16, LANES), jnp.float32)
    for c in range(C):
        for s in range(tsub):
            line = lane_sums(c, s)
            for j in range(4):
                line = line + poly[j][c : c + 1] * q_own[j][s : s + 1]
            out_m[c * tsub + s : c * tsub + s + 1, :] = line


def shards(source_coords, source_values, target_coords, target_owner):
    own_rows = source_coords.shape[1]
    own_tgt = target_coords.shape[1]
    n_grp = lax.axis_size("grp")
    n_blk = lax.axis_size("blk")
    sub = own_rows // LANES
    tsub = own_tgt // LANES
    slab_len = own_rows * n_grp
    root_n = math.sqrt(slab_len * n_blk)
    log2e = 1.0 / math.log(2.0)
    scale_x = math.sqrt(thin_factor * log2e)
    scale_y = math.sqrt(4.0 * slab_len * log2e)
    blk = lax.axis_index("blk")
    scales = jnp.array([[scale_x], [scale_y], [scale_y]], jnp.float32)
    shift = jnp.array([[0.0], [0.5], [0.5]], jnp.float32)
    pad = jnp.zeros((1, LANES), jnp.float32)
    own = jnp.concatenate(
        [
            ((source_coords - shift) * scales).reshape(3 * sub, LANES),
            pad,
            source_values.reshape(3 * sub, LANES),
            pad,
        ]
    )
    tgt = jnp.concatenate(
        [
            ((target_coords - shift) * scales).reshape(3 * tsub, LANES),
            (target_owner - blk).astype(jnp.float32).reshape(tsub, LANES),
        ]
    )
    peers = n_blk * n_grp
    near = (2 * REACH + 3) * n_grp
    inner = (2 * REACH + 1) * n_grp
    f32 = jnp.float32
    vmem = pl.BlockSpec(memory_space=pltpu.VMEM)
    out_w, out_m, out_p = pl.pallas_call(
        functools.partial(kernel, n_blk, n_grp, sub, tsub, scale_x, scale_y, root_n),
        out_shape=(
            jax.ShapeDtypeStruct((16, LANES), f32),
            jax.ShapeDtypeStruct((16, LANES), f32),
            jax.ShapeDtypeStruct((8, LANES), f32),
        ),
        in_specs=[vmem, vmem],
        out_specs=(vmem, vmem, vmem),
        scratch_shapes=[
            pltpu.VMEM((inner * sub, own_rows, LANES), f32),
            pltpu.VMEM((HELD * n_grp * sub, own_tgt, LANES), f32),
            pltpu.VMEM((3, own_rows, LANES), f32),
            pltpu.VMEM((4, own_tgt, LANES), f32),
            pltpu.VMEM((C, own_rows, LANES), f32),
            pltpu.VMEM((peers, 32, LANES), f32),
            pltpu.VMEM((peers, 16, LANES), f32),
            pltpu.VMEM((peers, 16, LANES), f32),
            pltpu.VMEM((peers, 1, LANES), f32),
            pltpu.VMEM((32, LANES), f32),
            pltpu.VMEM((16, LANES), f32),
            pltpu.VMEM((16, LANES), f32),
            pltpu.VMEM((1, LANES), f32),
            pltpu.VMEM((near, 16, LANES), f32),
            pltpu.VMEM((near, 16, LANES), f32),
            pltpu.VMEM((near, 16, LANES), f32),
            pltpu.VMEM((near, 16, LANES), f32),
            pltpu.VMEM((near, 16, LANES), f32),
            pltpu.SemaphoreType.DMA((4, 3)),
            pltpu.SemaphoreType.DMA((4, 3)),
        ],
        compiler_params=pltpu.CompilerParams(
            collective_id=0, has_side_effects=True, vmem_limit_bytes=63 * 1024 * 1024
        ),
    )(own, tgt)
    weights = out_w[: C * sub].reshape(C, own_rows)
    mapped = out_m[: C * tsub].reshape(C, own_tgt)
    return weights, out_p[:C, :4], mapped


def solution(mesh):
    return jax.shard_map(
        shards,
        mesh=mesh,
        in_specs=(
            P(None, ("blk", "grp")),
            P(None, ("blk", "grp")),
            P(None, ("blk", "grp")),
            P(("blk", "grp")),
        ),
        out_specs=(P(None, ("blk", "grp")), P(), P(None, ("blk", "grp"))),
        check_vma=False,
    )
```
